32 devices in a mesh: grp: 2 (over y), mode: 8 (over z, x), node: 2 (over core).
Axes of the slice: x: 2, y: 2, z: 4, core: 2. Of those that a mesh axis runs over, the one named last changes fastest.
Arguments:
- mode_basis: float32 [4096, 4096], P('mode', 'node'), may hold values from -6 to 6
- mode_scales: float32 [4096], P('mode'), may hold values from 0.003 to 0.02
- mean_log: float32 [4096], P(('node', 'mode')), may hold values from -0.5 to 0.5
- sample_seeds: int32 [4096], P('grp'), parts along dimension 0, may hold values from 0 to 1073741823
Outputs:
- modulus: float32 [4096, 4096], P(('node', 'mode'), 'grp'), parts along dimension 1
- sample_means: float32 [4096], P('grp'), parts along dimension 0
The draws below stay inside these ranges and needn't reach their ends.
There are 2 independent parts, one for each index of `grp`. The reference program is written for one: setup_inputs(seed, part) draws one part's arguments, and reference() takes and returns one part's arrays. A program takes and returns all parts, laid end to end along the dimension named above; an argument that names none is the same for every part. Nothing has to cross between parts.
All inputs are finite; a program needn't handle non-finite values.
Results may differ from the reference program's by a relative error of at most 0.00005.
Values sent between devices are 32-bit elements; how exact they have to be, the bound alone decides.
A program may use at most 64 MiB of HBM per device.

```python
import math
import jax
import jax.numpy as jnp
from jax import lax

MODES = 4096
SAMPLES = 2048
NODES = 4096


def plant(entries, own_key, smallest, top_value):
    spot = [jax.random.randint(jax.random.fold_in(own_key, axis), (), 0, length) for axis, length in enumerate(entries.shape)]
    widest = entries.shape.index(max(entries.shape))
    neighbour = spot[:widest] + [(spot[widest] + 1) % entries.shape[widest]] + spot[widest + 1:]
    return entries.at[tuple(spot)].set(smallest).at[tuple(neighbour)].set(top_value)


def with_spikes(array, own_key, source, target, blocks, factor):
    owner, partner = [(jnp.arange(array.shape[axis_at]) // (array.shape[axis_at] // blocks)).reshape([-1 if axis == axis_at else 1 for axis in range(array.ndim)]) for axis_at in (source, target)]
    chosen = jax.random.permutation(own_key, blocks)[partner]
    strong = (owner == chosen) | (owner == (partner + blocks // 2) % blocks)
    return jnp.where(strong, factor * array, array)


def level_of(stream_key, dims, split, low, high):
    loudness, own = 1.0, jax.random.fold_in(stream_key, 6)
    for axis_at, shards_of in split:
        draws = jnp.exp(jax.random.uniform(jax.random.fold_in(own, axis_at), (shards_of,), jnp.float32, low / len(split), high / len(split)))
        loudness = loudness * jnp.repeat(draws, dims[axis_at] // shards_of).reshape([-1 if axis == axis_at else 1 for axis in range(len(dims))])
    return loudness


def bell_draw_with(rng, shape, spread, reach, pieces, heavy, kind=jnp.bfloat16):
    entries = spread * jax.random.normal(rng, shape, jnp.float32)
    if pieces:
        entries = entries * level_of(rng, shape, pieces, -0.22, 0.18)
    return jnp.clip(with_spikes(entries, jax.random.fold_in(rng, 3), *heavy), -reach, reach).astype(kind)


def setup_inputs(seed: int = 0, part: int = 0) -> dict:
    key_of = jax.random.split(jax.random.key(seed), 5)
    own_keys = jax.random.split(jax.random.fold_in(key_of[4], part), 5)
    return {
        "mode_basis": bell_draw_with(key_of[0], (MODES, NODES), 1.0, 6.0, ((0, 8), (1, 2)), (0, 1, 8, 2.0), jnp.float32),
        "mode_scales": jnp.clip(jnp.exp(math.log(0.02) - 1.89712 * jax.random.uniform(key_of[1], (MODES,), jnp.float32) ** level_of(key_of[1], (MODES,), ((0, 8),), -0.2, 0.2)), 0.003, 0.02),
        "mean_log": jnp.clip(jax.random.uniform(key_of[2], (NODES,), jnp.float32, -0.5, 0.5) * level_of(key_of[2], (NODES,), ((0, 16),), -0.4, 0.0), -0.5, 0.5),
        "sample_seeds": plant(jax.random.randint(own_keys[3], (SAMPLES,), 0, 1073741824), jax.random.fold_in(own_keys[3], 1), 0, 1073741823).astype(jnp.int32),
    }


def scramble(seed_words, counter_words):
    mixed_word = seed_words * -1640531527 + counter_words * 668265261
    mixed_word = mixed_word ^ mixed_word >> 15 & 131071
    mixed_word = mixed_word * -2048144789
    mixed_word = mixed_word ^ mixed_word >> 13 & 524287
    mixed_word = mixed_word * -1028477387
    mixed_word = mixed_word ^ mixed_word >> 16 & 65535
    return mixed_word

def normals(sample_seeds, mode_start, mode_count):
    mode_ids = mode_start + jnp.arange(mode_count, dtype=jnp.int32)
    seed_words = sample_seeds.astype(jnp.int32)[None, :]
    counter_words = (2 * mode_ids).astype(jnp.int32)[:, None]
    first_word = scramble(seed_words, counter_words)
    second_word = scramble(seed_words, counter_words + 1)
    first_unit = ((first_word & 16777215).astype(jnp.float32) + 0.5) * (1.0 / 16777216.0)
    second_unit = ((second_word & 16777215).astype(jnp.float32) + 0.5) * (1.0 / 16777216.0)
    radius = jnp.sqrt(-2.0 * jnp.log(first_unit))
    return radius * jnp.cos(2.0 * math.pi * second_unit)

def reference(mode_basis, mode_scales, mean_log, sample_seeds):
    scaled = mode_scales[:, None] * mode_basis
    coeffs = normals(sample_seeds, 0, MODES)
    summed = lax.dot_general(scaled, coeffs, (((0,), (0,)), ((), ())), precision=lax.Precision.HIGHEST, preferred_element_type=jnp.float32)
    modulus = jnp.exp(mean_log[:, None] + summed)
    sample_means = lax.optimization_barrier(jnp.sum(modulus, axis=0)) / NODES
    return (modulus, sample_means)
```

```python
import functools
import math

import jax
import jax.numpy as jnp
import numpy as np
from jax import lax
from jax.experimental import pallas as pl
from jax.experimental.pallas import tpu as pltpu
from jax.sharding import PartitionSpec as P

MESH = pl.DeviceIdType.MESH


def sine_series():
    points = 0.25 * np.cos((np.arange(200) + 0.5) * np.pi / 400)
    powers = points[:, None] ** np.arange(0, 11, 2)[None, :]
    values = np.sin(2 * np.pi * points) / points
    return [float(c) for c in np.linalg.lstsq(powers, values, rcond=None)[0]]


SINE = sine_series()


def scramble(word):
    word = word ^ lax.shift_right_logical(word, jnp.int32(15))
    word = word * jnp.int32(-2048144789)
    word = word ^ lax.shift_right_logical(word, jnp.int32(13))
    word = word * jnp.int32(-1028477387)
    return word ^ lax.shift_right_logical(word, jnp.int32(16))


def normals(seed_terms, counter_terms):
    start_word = seed_terms + counter_terms
    first_word = scramble(start_word) & jnp.int32(16777215)
    second_word = scramble(start_word + jnp.int32(668265261)) & jnp.int32(16777215)
    first_unit = (first_word.astype(jnp.float32) + 0.5) * (1.0 / 16777216.0)
    square = -2.0 * jnp.log(first_unit)
    radius = square * lax.rsqrt(jnp.maximum(square, 1e-30))
    folded = jnp.abs(second_word.astype(jnp.float32) - 8388607.5) - 4194304.0
    turn = folded * (1.0 / 16777216.0)
    turn2 = turn * turn
    series = jnp.full_like(turn, SINE[-1])
    for coefficient in SINE[-2::-1]:
        series = series * turn2 + coefficient
    return (radius * turn) * series


def split(values):
    high = values.astype(jnp.bfloat16)
    return high, (values - high.astype(jnp.float32)).astype(jnp.bfloat16)


def kernel(n, basis, scales, mean, seeds, modulus, means, gathered, scale_all, mean_all, coefs, lhs,
           total, staged, parts, halves, net_send, net_recv, row_send, row_recv, core_send, core_recv,
           scale_send, scale_recv, part_send, part_recv, mean_sems, own_sem, out_sems, half_sems):
    g, me, c = lax.axis_index("grp"), lax.axis_index("mode"), lax.axis_index("node")
    _, _, pieces, piece, wide = gathered.shape
    rows = pieces * piece
    mine, theirs = [[side * 2 + p for p in range(2)] for side in (g, 1 - g)]
    samples = coefs.shape[-1]
    across, sibling = (1 - g, me, c), (g, me, 1 - c)

    def to(step):
        flipped, bit = 0, 1
        while bit < n:
            flipped = flipped + lax.rem(me // bit + step // bit, 2) * bit
            bit *= 2
        return flipped

    near, quarter, eighth = n // 2, n // 4, n // 8
    inner = lax.rem(me // near + me // quarter, 2)

    def far(q):
        return near + quarter - 1 - q // 2 + lax.rem(q, 2) * quarter

    def relay(j):
        base = n - 1 - j
        return base + inner * (quarter * (1 - 2 * ((base // quarter) % 2)))

    def each(low, high, body):
        if high - low == 1:
            body(low)
        else:
            pl.loop(low, high)(body)

    barrier = pltpu.get_barrier_semaphore()

    @pl.loop(1, n)
    def _(step):
        pl.semaphore_signal(barrier, inc=1, device_id=(g, to(step), c), device_id_type=MESH)

    pl.semaphore_signal(barrier, inc=1, device_id=across, device_id_type=MESH)
    pl.semaphore_signal(barrier, inc=1, device_id=sibling, device_id_type=MESH)

    own_scale = scale_all.at[me]
    own_mean = mean_all.at[c]
    own_scale[...] = scales[...]
    own_mean[...] = mean[...]
    own_columns = pl.ds(pl.multiple_of(me * wide, 128), wide)
    own = [
        pltpu.make_async_copy(basis.at[pl.ds(k * piece, piece), own_columns], gathered.at[c, me, k], own_sem.at[k])
        for k in range(pieces)
    ]
    for copy in own:
        copy.start()
    pl.semaphore_wait(barrier, n + 1)

    def net(step, owner, k):
        peer = to(step)
        return pltpu.make_async_remote_copy(
            src_ref=basis.at[pl.ds(pl.multiple_of(k * piece, 8), piece), pl.ds(pl.multiple_of(peer * wide, 128), wide)],
            dst_ref=gathered.at[c, owner, k],
            send_sem=net_send.at[k, step], recv_sem=net_recv.at[k, step], device_id=(g, peer, c), device_id_type=MESH)

    def scale_copy(step, owner):
        return pltpu.make_async_remote_copy(
            src_ref=scales, dst_ref=scale_all.at[owner],
            send_sem=scale_send.at[step], recv_sem=scale_recv.at[step], device_id=(g, to(step), c), device_id_type=MESH)

    def row_copy(step, owner, k, p):
        block = gathered.at[c, owner, k]
        return pltpu.make_async_remote_copy(
            src_ref=block, dst_ref=block,
            send_sem=row_send.at[p, step], recv_sem=row_recv.at[p, step], device_id=across, device_id_type=MESH)

    def core_copy(step, owner, k, side):
        block = gathered.at[side, owner, k]
        return pltpu.make_async_remote_copy(
            src_ref=block, dst_ref=block,
            send_sem=core_send.at[k, step], recv_sem=core_recv.at[k, step],
            device_id=sibling, device_id_type=MESH)

    def part_copy(step, owner):
        return pltpu.make_async_remote_copy(
            src_ref=parts.at[me], dst_ref=parts.at[owner],
            send_sem=part_send.at[step], recv_sem=part_recv.at[step], device_id=(g, to(step), c), device_id_type=MESH)

    mean_copy = lambda side: pltpu.make_async_remote_copy(
        src_ref=mean, dst_ref=mean_all.at[side], send_sem=mean_sems.at[0], recv_sem=mean_sems.at[1],
        device_id=sibling, device_id_type=MESH)

    @pl.loop(1, n)
    def _(step):
        scale_copy(step, me).start()

    mean_copy(c).start()

    @pl.loop(0, near)
    def _(q):
        for k in mine:
            net(far(q), me, k).start()

    @pl.loop(quarter, near)
    def _(step):
        for k in range(pieces):
            net(step, me, k).start()

    @pl.loop(1, quarter)
    def _(step):
        for k in range(pieces):
            net(step, me, k).start()

    for copy in own:
        copy.wait()
    for k in range(pieces):
        core_copy(0, me, k, c).start()

    seed_terms = seeds[:, pl.ds(pl.multiple_of(c * samples, 128), samples)] * jnp.int32(-1640531527)
    lanes = min(512, samples)

    half = rows // 2
    tiles = half // 16

    def draw_half(owner, side):
        @pl.loop(0, tiles)
        def _(tile):
            first = owner * rows + side * half + tile * 16
            ids = lax.broadcasted_iota(jnp.int32, (16, lanes), 0) + first
            counters = ids * jnp.int32(2 * 668265261 - 2**32 if 2 * 668265261 >= 2**31 else 2 * 668265261)
            for start in range(0, samples, lanes):
                high, low = split(normals(seed_terms[:, start:start + lanes], counters))
                for part, values in enumerate((high, low, high)):
                    here = pl.ds(pl.multiple_of((3 * side + part) * half + tile * 16, 16), 16)
                    coefs[owner, here, start:start + lanes] = values

    def draw(owner):
        draw_half(owner, 0)
        draw_half(owner, 1)

    def accumulate(owner, first_row, depth, first):
        columns = min(1024, samples)

        @pl.loop(0, samples // columns)
        def _(tile):
            here = pl.ds(pl.multiple_of(tile * columns, 128), columns)
            product = jnp.dot(lhs[:, 0:depth], coefs[owner, pl.ds(first_row, depth), here], preferred_element_type=jnp.float32)
            if first:
                total[:, here] = product
            else:
                total[:, here] += product

    def multiply(step, owner, first):
        for k in range(pieces):
            core_copy(step, owner, k, 1 - c).wait_recv()
        for side in range(2):
            block = gathered[side, owner].reshape(rows, wide)
            high, low = split(block.T * scale_all[owner])
            for h in range(2):
                for part, values in enumerate((high, high, low)):
                    at = (3 * h + part) * half
                    lhs[side * wide:(side + 1) * wide, at:at + half] = values[:, h * half:(h + 1) * half]
        accumulate(owner, 0, 3 * rows, first)

    def multiply_half(step, h, ks):
        owner = to(step)
        for k in ks:
            core_copy(step, owner, k, 1 - c).wait_recv()
        scale_row = jnp.where(h == 0, scale_all[owner][:, 0:half], scale_all[owner][:, half:rows])
        for side in range(2):
            block = gathered[side, owner, pl.ds(h * (pieces // 2), pieces // 2)].reshape(half, wide)
            high, low = split(block.T * scale_row)
            for part, values in enumerate((high, high, low)):
                lhs[side * wide:(side + 1) * wide, part * half:(part + 1) * half] = values
        accumulate(owner, pl.multiple_of(h * (3 * half), 16), 3 * half, False)

    def forward(j, p):
        step = relay(j)
        owner, k = to(step), mine[p]
        net(step, owner, k).wait_recv()
        row_copy(step, owner, k, p).start()
        core_copy(step, owner, k, c).start()

    def finish(j, p):
        step = relay(j)
        owner, k = to(step), theirs[p]
        row_copy(step, owner, k, p).wait_recv()
        core_copy(step, owner, k, c).start()

    def share(step):
        for k in range(pieces):
            net(step, to(step), k).wait_recv()
            core_copy(step, to(step), k, c).start()

    def use(step):
        scale_copy(step, to(step)).wait_recv()
        multiply(step, to(step), False)

    def group(index):
        return index * eighth, (index + 1) * eighth

    draw(me)
    each(1, quarter, lambda step: draw(to(step)))
    multiply(0, me, True)
    each(*group(0), lambda j: draw(to(relay(j))))
    each(*group(0), lambda j: forward(j, 0))
    each(*group(1), lambda j: draw_half(to(relay(j)), 0))
    each(*group(0), lambda j: forward(j, 1))
    each(*group(1), lambda j: draw_half(to(relay(j)), 1))
    each(*group(2), lambda step: draw_half(to(step), 0))
    each(*group(0), lambda j: finish(j, 0))
    each(*group(2), lambda step: draw_half(to(step), 1))
    each(*group(0), lambda j: finish(j, 1))
    each(1, quarter, share)
    each(1, quarter, use)
    each(*group(0), lambda j: use(relay(j)))
    each(*group(1), lambda j: forward(j, 0))
    each(*group(2), lambda j: draw_half(to(relay(j)), 0))
    each(*group(1), lambda j: forward(j, 1))
    each(*group(2), lambda j: draw_half(to(relay(j)), 1))
    each(*group(1), lambda j: finish(j, 0))
    each(*group(3), lambda step: draw_half(to(step), 0))
    each(*group(1), lambda j: finish(j, 1))
    each(*group(3), lambda step: draw_half(to(step), 1))
    each(*group(1), lambda j: use(relay(j)))
    each(*group(2), lambda j: forward(j, 0))
    each(*group(3), lambda j: draw_half(to(relay(j)), 0))
    each(*group(2), lambda j: forward(j, 1))
    each(*group(3), lambda j: draw_half(to(relay(j)), 1))
    each(*group(2), share)
    for p in range(2):
        each(*group(2), lambda j: finish(j, p))
    each(*group(2), use)
    each(*group(3), lambda j: forward(j, 0))
    each(*group(2), lambda j: use(relay(j)))
    each(*group(3), lambda j: forward(j, 1))
    each(*group(3), share)
    each(*group(3), use)

    def use_mine(j):
        scale_copy(relay(j), to(relay(j))).wait_recv()
        multiply_half(relay(j), g, mine)

    each(*group(3), use_mine)
    for p in range(2):
        each(*group(3), lambda j: finish(j, p))
    each(*group(3), lambda j: multiply_half(relay(j), 1 - g, theirs))

    mean_copy(1 - c).wait_recv()

    sums = jnp.zeros((1, samples), jnp.float32)
    for side in range(2):
        shift = jnp.broadcast_to(mean_all[side], (8, wide)).T[:, :1]
        values = jnp.exp(total[side * wide:(side + 1) * wide, :] + shift)
        staged[side] = values
        sums = sums + jnp.sum(values, axis=0, keepdims=True)
    parts[me] = sums
    out_columns = modulus.at[:, pl.ds(pl.multiple_of(c * samples, 128), samples)]
    other_columns = modulus.at[:, pl.ds(pl.multiple_of((1 - c) * samples, 128), samples)]
    local_out = pltpu.make_async_copy(staged.at[c], out_columns, out_sems.at[0])
    send_out = lambda landing: pltpu.make_async_remote_copy(
        src_ref=staged.at[1 - c], dst_ref=landing, send_sem=out_sems.at[1], recv_sem=out_sems.at[2],
        device_id=sibling, device_id_type=MESH)

    @pl.loop(1, n)
    def _(step):
        part_copy(step, me).start()

    send_out(out_columns).start()
    local_out.start()

    @pl.loop(1, n)
    def _(step):
        part_copy(step, to(step)).wait_recv()

    summed = jnp.zeros((1, samples), jnp.float32)
    for m in range(n):
        summed = summed + parts[m]
    halves[c] = summed / (n * 2 * wide)
    half_copy = lambda side: pltpu.make_async_remote_copy(
        src_ref=halves.at[c], dst_ref=halves.at[side], send_sem=half_sems.at[0], recv_sem=half_sems.at[1],
        device_id=sibling, device_id_type=MESH)
    half_copy(c).start()

    mean_copy(c).wait_send()
    for k in range(pieces):
        core_copy(0, me, k, c).wait_send()

    @pl.loop(1, n)
    def _(step):
        scale_copy(step, me).wait_send()
        part_copy(step, me).wait_send()
        for k in range(pieces):
            core_copy(step, to(step), k, c).wait_send()
        for k in mine:
            net(step, me, k).wait_send()

    @pl.loop(1, near)
    def _(step):
        for k in theirs:
            net(step, me, k).wait_send()

    @pl.loop(near, n)
    def _(step):
        for p, k in enumerate(mine):
            row_copy(step, to(step), k, p).wait_send()

    half_copy(1 - c).wait_recv()
    half_copy(c).wait_send()
    means[:, 0:samples] = halves[0]
    means[:, samples:2 * samples] = halves[1]
    local_out.wait()
    send_out(other_columns).wait_recv()
    send_out(out_columns).wait_send()


def on_device(mode_basis, mode_scales, mean_log, sample_seeds):
    n = lax.axis_size("mode")
    rows, wide, all_samples = mode_scales.shape[0], mean_log.shape[0], sample_seeds.shape[0]
    piece, samples = rows // 4, all_samples // 2
    vmem = pl.BlockSpec(memory_space=pltpu.VMEM)
    anywhere = pl.BlockSpec(memory_space=pl.ANY)
    dma = pltpu.SemaphoreType.DMA
    modulus, means = pl.pallas_call(
        functools.partial(kernel, n),
        out_shape=(
            jax.ShapeDtypeStruct((wide, all_samples), jnp.float32),
            jax.ShapeDtypeStruct((1, all_samples), jnp.float32),
        ),
        in_specs=[anywhere, vmem, vmem, vmem],
        out_specs=(anywhere, vmem),
        scratch_shapes=[
            pltpu.VMEM((2, n, 4, piece, wide), jnp.float32),
            pltpu.VMEM((n, 1, rows), jnp.float32),
            pltpu.VMEM((2, 1, wide), jnp.float32),
            pltpu.VMEM((n, 3 * rows, samples), jnp.bfloat16),
            pltpu.VMEM((2 * wide, 3 * rows), jnp.bfloat16),
            pltpu.VMEM((2 * wide, samples), jnp.float32),
            pltpu.VMEM((2, wide, samples), jnp.float32),
            pltpu.VMEM((n, 1, samples), jnp.float32),
            pltpu.VMEM((2, 1, samples), jnp.float32),
            dma((4, n)), dma((4, n)), dma((2, n)), dma((2, n)), dma((4, n)), dma((4, n)),
            dma((n,)), dma((n,)), dma((n,)), dma((n,)), dma((2,)), dma((4,)), dma((3,)), dma((2,)),
        ],
        compiler_params=pltpu.CompilerParams(
            collective_id=0, has_side_effects=True, vmem_limit_bytes=60 * 1024 * 1024
        ),
    )(mode_basis, mode_scales[None, :], mean_log[None, :], sample_seeds[None, :])
    return modulus, means[0]


def solution(mesh):
    return jax.shard_map(
        on_device,
        mesh=mesh,
        in_specs=(P("mode", "node"), P("mode"), P(("node", "mode")), P("grp")),
        out_specs=(P(("node", "mode"), "grp"), P("grp")),
        check_vma=False,
    )
```

```python
import functools
import math

import jax
import jax.numpy as jnp
import numpy as np
from jax import lax
from jax.experimental import pallas as pl
from jax.experimental.pallas import tpu as pltpu
from jax.sharding import PartitionSpec as P

MESH = pl.DeviceIdType.MESH
PIECES = 8


def sine_series():
    points = 0.25 * np.cos((np.arange(200) + 0.5) * np.pi / 400)
    powers = points[:, None] ** np.arange(0, 9, 2)[None, :]
    values = np.sin(2 * np.pi * points) / points
    return [float(c) for c in np.linalg.lstsq(powers, values, rcond=None)[0]]


SINE = sine_series()


def scramble(word):
    word = word ^ lax.shift_right_logical(word, jnp.int32(15))
    word = word * jnp.int32(-2048144789)
    word = word ^ lax.shift_right_logical(word, jnp.int32(13))
    word = word * jnp.int32(-1028477387)
    return word ^ lax.shift_right_logical(word, jnp.int32(16))


def normals(seed_terms, counter_terms):
    start_word = seed_terms + counter_terms
    first_word = scramble(start_word) & jnp.int32(16777215)
    second_word = scramble(start_word + jnp.int32(668265261)) & jnp.int32(16777215)
    first_unit = (first_word.astype(jnp.float32) + 0.5) * (1.0 / 16777216.0)
    square = -2.0 * jnp.log(first_unit)
    radius = square * lax.rsqrt(jnp.maximum(square, 1e-30))
    folded = jnp.abs(second_word.astype(jnp.float32) - 8388607.5) - 4194304.0
    turn = folded * (1.0 / 16777216.0)
    turn2 = turn * turn
    series = jnp.full_like(turn, SINE[-1])
    for coefficient in SINE[-2::-1]:
        series = series * turn2 + coefficient
    return (radius * turn) * series


def split(values):
    high = values.astype(jnp.bfloat16)
    return high, (values - high.astype(jnp.float32)).astype(jnp.bfloat16)


def kernel(n, basis, scales, mean, seeds, modulus, means, gathered, scale_all, mean_all, seed_row, coefs, lhs,
           total, staged, parts, near_recv, far_recv, extra_recv, net_send, row_recv, row_send, core_recv, core_send,
           scale_send, scale_recv, mean_sems, own_sem, part_recv, part_send, out_sems, small_sems):
    g, me, c = lax.axis_index("grp"), lax.axis_index("mode"), lax.axis_index("node")
    _, _, pieces, piece, wide = gathered.shape
    rows, deep = pieces * piece, pieces // 2
    half = rows // 2
    last = deep - 1
    samples = coefs.shape[-1]
    across, sibling = (1 - g, me, c), (g, me, 1 - c)
    mine, theirs = [[side * deep + p for p in range(deep)] for side in (g, 1 - g)]

    def to(step):
        flipped, bit = 0, 1
        while bit < n:
            flipped = flipped + lax.rem(me // bit + step // bit, 2) * bit
            bit *= 2
        return flipped

    near, quarter, eighth = n // 2, n // 4, n // 8
    inner = lax.rem(me // near + me // quarter, 2)

    def far(q):
        return near + quarter - 1 - q // 2 + lax.rem(q, 2) * quarter

    def relay(j):
        base = n - 1 - j
        return base + inner * (quarter * (1 - 2 * ((base // quarter) % 2)))

    def each(low, high, body):
        if high - low == 1:
            body(low)
        else:
            pl.loop(low, high)(body)

    def group(index):
        return index * eighth, (index + 1) * eighth

    def outside(*actions):
        @pl.when(inner == 0)
        def _():
            for action in actions:
                action()

    def inside(*actions):
        @pl.when(inner == 1)
        def _():
            for action in actions:
                action()

    def settle(block, sem):
        pltpu.make_async_copy(block, block, sem).wait()

    barrier = pltpu.get_barrier_semaphore()

    @pl.loop(1, n)
    def _(step):
        pl.semaphore_signal(barrier, inc=1, device_id=(g, to(step), c), device_id_type=MESH)
        pl.semaphore_signal(barrier, inc=1, device_id=(g, to(step), 1 - c), device_id_type=MESH)

    pl.semaphore_signal(barrier, inc=1, device_id=across, device_id_type=MESH)
    pl.semaphore_signal(barrier, inc=1, device_id=sibling, device_id_type=MESH)

    small = [
        pltpu.make_async_copy(scales, scale_all.at[me], small_sems.at[0]),
        pltpu.make_async_copy(mean, mean_all.at[c], small_sems.at[1]),
        pltpu.make_async_copy(seeds.at[:, pl.ds(pl.multiple_of(c * samples, 128), samples)], seed_row, small_sems.at[2]),
    ]
    for copy in small:
        copy.start()
    own_columns = pl.ds(pl.multiple_of(me * wide, 128), wide)
    for k in range(pieces):
        pltpu.make_async_copy(
            basis.at[pl.ds(k * piece, piece), own_columns], gathered.at[c, me, k], own_sem.at[0]).start()
    for copy in small:
        copy.wait()
    pl.semaphore_wait(barrier, 2 * n)

    def net(step, owner, k, send_sem, recv_sem):
        peer = to(step)
        return pltpu.make_async_remote_copy(
            src_ref=basis.at[pl.ds(pl.multiple_of(k * piece, 8), piece), pl.ds(pl.multiple_of(peer * wide, 128), wide)],
            dst_ref=gathered.at[c, owner, k],
            send_sem=send_sem, recv_sem=recv_sem, device_id=(g, peer, c), device_id_type=MESH)

    def far_copy(step, owner, p):
        return net(step, owner, mine[p], net_send.at[0], far_recv.at[p, step - near])

    def near_copy(step, owner, k):
        return net(step, owner, k, net_send.at[1], near_recv.at[k // deep, step])

    def extra_copy(j, owner):
        return net(relay(j), owner, theirs[last], net_send.at[2], extra_recv.at[j - 3 * eighth])

    def scale_copy(step, owner):
        return pltpu.make_async_remote_copy(
            src_ref=scale_all.at[me], dst_ref=scale_all.at[owner],
            send_sem=scale_send.at[0], recv_sem=scale_recv.at[step], device_id=(g, to(step), c), device_id_type=MESH)

    def row_copy(j, owner, p):
        block = gathered.at[c, owner, mine[p]]
        sem = row_send.at[(j - 3 * eighth + near) // near]
        return pltpu.make_async_remote_copy(
            src_ref=block, dst_ref=block,
            send_sem=sem, recv_sem=row_recv.at[2 * p // deep, relay(j) - near], device_id=across, device_id_type=MESH)

    def core_copy(step, owner, k, h, side):
        block = gathered.at[side, owner, k]
        return pltpu.make_async_remote_copy(
            src_ref=block, dst_ref=block,
            send_sem=core_send.at[0], recv_sem=core_recv.at[h, step],
            device_id=sibling, device_id_type=MESH)

    def part_copy(step, owner, source, target):
        return pltpu.make_async_remote_copy(
            src_ref=parts.at[c, me], dst_ref=parts.at[source, owner],
            send_sem=part_send.at[lax.rem(target + c, 2)], recv_sem=part_recv.at[lax.rem(source + target, 2)],
            device_id=(g, to(step), target), device_id_type=MESH)

    mean_copy = lambda side: pltpu.make_async_remote_copy(
        src_ref=mean_all.at[c], dst_ref=mean_all.at[side], send_sem=mean_sems.at[0], recv_sem=mean_sems.at[1],
        device_id=sibling, device_id_type=MESH)

    @pl.loop(1, n)
    def _(step):
        scale_copy(step, me).start()

    mean_copy(c).start()

    @pl.loop(0, near)
    def _(q):
        for p in range(deep):
            far_copy(far(q), me, p).start()

    inside(lambda: each(*group(3), lambda j: extra_copy(j, me).start()))

    @pl.loop(quarter, near)
    def _(step):
        for k in range(pieces):
            near_copy(step, me, k).start()

    @pl.loop(1, quarter)
    def _(step):
        for k in range(pieces):
            near_copy(step, me, k).start()

    settle(gathered.at[c, me], own_sem.at[0])
    for k in range(pieces):
        core_copy(0, me, k, k // deep, c).start()

    seed_terms = seed_row[...] * jnp.int32(-1640531527)
    lanes = min(512, samples)
    tiles = half // 16

    def draw_half(owner, side):
        @pl.loop(0, tiles)
        def _(tile):
            first = owner * rows + side * half + tile * 16
            ids = lax.broadcasted_iota(jnp.int32, (16, lanes), 0) + first
            counters = ids * jnp.int32(2 * 668265261 - 2**32 if 2 * 668265261 >= 2**31 else 2 * 668265261)
            for start in range(0, samples, lanes):
                high, low = split(normals(seed_terms[:, start:start + lanes], counters))
                for part, values in enumerate((high, low, high)):
                    here = pl.ds(pl.multiple_of((3 * side + part) * half + tile * 16, 16), 16)
                    coefs[owner, here, start:start + lanes] = values

    def draw(owner):
        draw_half(owner, 0)
        draw_half(owner, 1)

    def accumulate(owner, first_row, depth, first):
        columns = min(1024, samples)

        @pl.loop(0, samples // columns)
        def _(tile):
            here = pl.ds(pl.multiple_of(tile * columns, 128), columns)
            product = jnp.dot(lhs[:, 0:depth], coefs[owner, pl.ds(first_row, depth), here], preferred_element_type=jnp.float32)
            if first:
                total[:, here] = product
            else:
                total[:, here] += product

    def scaled(step):
        scale_copy(step, to(step)).wait_recv()
        return step

    def arrived(step, owner, h):
        settle(gathered.at[1 - c, owner, pl.ds(h * deep, deep)], core_recv.at[h, step])

    def multiply(step, first):
        owner = to(step)
        for h in range(2):
            arrived(step, owner, h)
        for side in range(2):
            block = gathered[side, owner].reshape(rows, wide)
            high, low = split(block.T * scale_all[owner])
            for h in range(2):
                for part, values in enumerate((high, high, low)):
                    at = (3 * h + part) * half
                    lhs[side * wide:(side + 1) * wide, at:at + half] = values[:, h * half:(h + 1) * half]
        accumulate(owner, 0, 3 * rows, first)

    def multiply_half(step, h):
        owner = to(step)
        arrived(step, owner, h)
        scale_row = jnp.where(h == 0, scale_all[owner][:, 0:half], scale_all[owner][:, half:rows])
        for side in range(2):
            block = gathered[side, owner, pl.ds(h * deep, deep)].reshape(half, wide)
            high, low = split(block.T * scale_row)
            for part, values in enumerate((high, high, low)):
                lhs[side * wide:(side + 1) * wide, part * half:(part + 1) * half] = values
        accumulate(owner, pl.multiple_of(h * (3 * half), 16), 3 * half, False)

    def forward(j, p, relayed=True):
        step = relay(j)
        owner = to(step)
        far_copy(step, owner, p).wait_recv()
        if relayed:
            row_copy(j, owner, p).start()
        core_copy(step, owner, mine[p], g, c).start()

    def finish(j, ps, relayed):
        step = relay(j)
        owner = to(step)
        settle(gathered.at[c, owner, pl.ds(theirs[ps[0]], relayed)], row_recv.at[2 * ps[0] // deep, step - near])
        if relayed < len(ps):
            extra_copy(j, owner).wait_recv()
        for p in ps:
            core_copy(step, owner, theirs[p], 1 - g, c).start()

    def forwards(index, *ps):
        for p in ps:
            each(*group(index), lambda j: forward(j, p))

    def forward_last(index):
        each(*group(index), lambda j: forward(j, last, False))

    def finishes(index, *halves, relayed=deep // 2):
        for ps in halves:
            each(*group(index), lambda j: finish(j, ps, relayed))

    def share(step, h):
        owner = to(step)
        settle(gathered.at[c, owner, pl.ds(h * deep, deep)], near_recv.at[h, step])
        for k in range(h * deep, (h + 1) * deep):
            core_copy(step, owner, k, h, c).start()

    def share_near(index, *hs):
        for h in hs:
            each(*group(index), lambda step: share(step, h))

    def draw_far(index, side):
        each(*group(index), lambda j: draw_half(to(relay(j)), side))

    def draw_near(index, side):
        each(*group(index), lambda step: draw_half(to(step), side))

    def use_far(index):
        each(*group(index), lambda j: multiply(scaled(relay(j)), False))

    def use_near(index, h):
        each(*group(index), lambda step: multiply_half(step if h else scaled(step), h))

    def use_mine(index):
        each(*group(index), lambda j: multiply_half(scaled(relay(j)), g))

    def use_theirs(index):
        each(*group(index), lambda j: multiply_half(relay(j), 1 - g))

    early, late = tuple(range(deep // 2)), tuple(range(deep // 2, deep))
    draw(me)
    each(1, quarter, lambda step: draw(to(step)))
    multiply(0, True)
    inside(lambda: forwards(0, *early, *late))
    draw_far(0, 0)
    outside(lambda: forwards(0, *early))
    draw_far(0, 1)
    draw_far(1, 0)
    outside(lambda: forwards(0, *late))
    inside(lambda: finishes(0, early))
    draw_far(1, 1)
    outside(lambda: finishes(0, early))
    inside(lambda: finishes(0, late), lambda: forwards(1, *early))
    draw_near(2, 0)
    inside(lambda: forwards(1, *late))
    for h in range(2):
        each(1, quarter, lambda step: share(step, h))
    draw_near(2, 1)
    outside(lambda: finishes(0, late), lambda: forwards(1, *early))
    each(1, quarter, lambda step: multiply(scaled(step), False))
    inside(lambda: finishes(1, early))
    use_far(0)
    outside(lambda: forwards(1, *late))
    inside(lambda: finishes(1, late))
    draw_far(2, 0)
    outside(lambda: forwards(2, 0))
    draw_far(2, 1)
    outside(lambda: forwards(2, 1, 2), lambda: finishes(1, early))
    draw_near(3, 0)
    outside(lambda: forwards(2, 3), lambda: finishes(1, late))
    draw_near(3, 1)
    inside(lambda: forwards(2, *early))
    use_far(1)
    inside(lambda: forwards(2, 2))
    draw_far(3, 0)
    inside(lambda: forwards(2, 3))
    share_near(2, 0, 1)
    draw_far(3, 1)
    outside(lambda: finishes(2, early, late), lambda: forwards(3, 0, 1, 2))
    use_near(2, 0)
    outside(lambda: forwards(3, 3))
    use_near(2, 1)
    use_mine(2)
    inside(lambda: forwards(3, 0), lambda: finishes(2, early, late))
    share_near(3, 0)
    inside(lambda: forwards(3, 1))
    use_near(3, 0)
    inside(lambda: forwards(3, 2))
    use_theirs(2)
    inside(lambda: forward_last(3))
    outside(lambda: finishes(3, early))
    inside(lambda: share_near(3, 1), lambda: finishes(3, early))
    use_mine(3)
    outside(lambda: finishes(3, late), lambda: share_near(3, 1))
    inside(lambda: finishes(3, late, relayed=deep // 2 - 1))
    use_near(3, 1)
    use_theirs(3)

    mean_copy(1 - c).wait_recv()

    sums = jnp.zeros((1, samples), jnp.float32)
    for side in range(2):
        shift = jnp.broadcast_to(mean_all[side], (8, wide)).T[:, :1]
        values = jnp.exp(total[side * wide:(side + 1) * wide, :] + shift)
        staged[side] = values
        sums = sums + jnp.sum(values, axis=0, keepdims=True)
    parts[c, me] = sums
    out_columns = modulus.at[:, pl.ds(pl.multiple_of(c * samples, 128), samples)]
    other_columns = modulus.at[:, pl.ds(pl.multiple_of((1 - c) * samples, 128), samples)]
    local_out = pltpu.make_async_copy(staged.at[c], out_columns, out_sems.at[0])
    send_out = lambda landing: pltpu.make_async_remote_copy(
        src_ref=staged.at[1 - c], dst_ref=landing, send_sem=out_sems.at[1], recv_sem=out_sems.at[2],
        device_id=sibling, device_id_type=MESH)

    @pl.loop(1, n)
    def _(step):
        part_copy(step, me, c, c).start()
        part_copy(step, me, c, 1 - c).start()

    part_copy(0, me, c, 1 - c).start()
    send_out(out_columns).start()
    local_out.start()

    mean_copy(c).wait_send()
    settle(scale_all.at[0:n - 1], scale_send.at[0])
    settle(gathered.at[0, 0:near, 0:deep], net_send.at[0])
    settle(gathered.at[0, 0:near - 1], net_send.at[1])
    settle(gathered.at[0], core_send.at[0])
    settle(gathered.at[0, 0:3 * eighth, 0:deep], row_send.at[0])
    outside(lambda: settle(gathered.at[0, 0:eighth, 0:deep], row_send.at[1]))
    inside(lambda: settle(gathered.at[0, 0:eighth, 0:last], row_send.at[1]),
           lambda: settle(gathered.at[0, 0:eighth, 0], net_send.at[2]))
    settle(parts.at[0, 0:n - 1], part_send.at[0])
    settle(parts.at[0], part_send.at[1])
    settle(parts.at[0, 0:n - 1], part_recv.at[0])
    settle(parts.at[0], part_recv.at[1])

    for side in range(2):
        summed = jnp.zeros((1, samples), jnp.float32)
        for m in range(n):
            summed = summed + parts[side, m]
        means[:, side * samples:(side + 1) * samples] = summed / (n * 2 * wide)
    local_out.wait()
    send_out(other_columns).wait_recv()
    send_out(out_columns).wait_send()


def on_device(mode_basis, mode_scales, mean_log, sample_seeds):
    n = lax.axis_size("mode")
    rows, wide, all_samples = mode_scales.shape[0], mean_log.shape[0], sample_seeds.shape[0]
    piece, samples, near = rows // PIECES, all_samples // 2, n // 2
    vmem = pl.BlockSpec(memory_space=pltpu.VMEM)
    anywhere = pl.BlockSpec(memory_space=pl.ANY)
    dma = pltpu.SemaphoreType.DMA
    modulus, means = pl.pallas_call(
        functools.partial(kernel, n),
        out_shape=(
            jax.ShapeDtypeStruct((wide, all_samples), jnp.float32),
            jax.ShapeDtypeStruct((1, all_samples), jnp.float32),
        ),
        in_specs=[anywhere] * 4,
        out_specs=(anywhere, vmem),
        scratch_shapes=[
            pltpu.VMEM((2, n, PIECES, piece, wide), jnp.float32),
            pltpu.VMEM((n, 1, rows), jnp.float32),
            pltpu.VMEM((2, 1, wide), jnp.float32),
            pltpu.VMEM((1, samples), jnp.int32),
            pltpu.VMEM((n, 3 * rows, samples), jnp.bfloat16),
            pltpu.VMEM((2 * wide, 3 * rows), jnp.bfloat16),
            pltpu.VMEM((2 * wide, samples), jnp.float32),
            pltpu.VMEM((2, wide, samples), jnp.float32),
            pltpu.VMEM((2, n, 1, samples), jnp.float32),
            dma((2, near)), dma((PIECES // 2, near)), dma((n // 8,)), dma((3,)), dma((2, near)), dma((2,)), dma((2, n)), dma((1,)),
            dma((1,)), dma((n,)), dma((2,)), dma((1,)), dma((2,)), dma((2,)), dma((3,)), dma((3,)),
        ],
        compiler_params=pltpu.CompilerParams(
            collective_id=0, has_side_effects=True, vmem_limit_bytes=60 * 1024 * 1024
        ),
    )(mode_basis, mode_scales[None, :], mean_log[None, :], sample_seeds[None, :])
    return modulus, means[0]


def solution(mesh):
    return jax.shard_map(
        on_device,
        mesh=mesh,
        in_specs=(P("mode", "node"), P("mode"), P(("node", "mode")), P("grp")),
        out_specs=(P(("node", "mode"), "grp"), P("grp")),
        check_vma=False,
    )
```

```python
import functools
import math

import jax
import jax.numpy as jnp
import numpy as np
from jax import lax
from jax.experimental import pallas as pl
from jax.experimental.pallas import tpu as pltpu
from jax.sharding import PartitionSpec as P

MESH = pl.DeviceIdType.MESH
PIECES = 8


def sine_series():
    points = 0.25 * np.cos((np.arange(200) + 0.5) * np.pi / 400)
    powers = points[:, None] ** np.arange(0, 9, 2)[None, :]
    values = np.sin(2 * np.pi * points) / points
    return [float(c) for c in np.linalg.lstsq(powers, values, rcond=None)[0]]


SINE = sine_series()


def scramble(word):
    word = word ^ lax.shift_right_logical(word, jnp.int32(15))
    word = word * jnp.int32(-2048144789)
    word = word ^ lax.shift_right_logical(word, jnp.int32(13))
    word = word * jnp.int32(-1028477387)
    return word ^ lax.shift_right_logical(word, jnp.int32(16))


def normals(seed_terms, counter_terms):
    start_word = seed_terms + counter_terms
    first_word = scramble(start_word) & jnp.int32(16777215)
    second_word = scramble(start_word + jnp.int32(668265261)) & jnp.int32(16777215)
    first_unit = (first_word.astype(jnp.float32) + 0.5) * (1.0 / 16777216.0)
    square = -2.0 * jnp.log(first_unit)
    radius = square * lax.rsqrt(jnp.maximum(square, 1e-30))
    folded = jnp.abs(second_word.astype(jnp.float32) - 8388607.5) - 4194304.0
    turn = folded * (1.0 / 16777216.0)
    turn2 = turn * turn
    series = jnp.full_like(turn, SINE[-1])
    for coefficient in SINE[-2::-1]:
        series = series * turn2 + coefficient
    return (radius * turn) * series


def split(values):
    high = values.astype(jnp.bfloat16)
    return high, (values - high.astype(jnp.float32)).astype(jnp.bfloat16)


def kernel(n, basis, scales, mean, seeds, modulus, means, gathered, scale_all, mean_all, seed_row, coefs, lhs,
           total, staged, parts, near_recv, far_recv, extra_recv, net_send, row_recv, row_send, core_recv, core_send,
           scale_send, scale_recv, mean_sems, own_sem, part_recv, part_send, out_sems, small_sems):
    g, me, c = lax.axis_index("grp"), lax.axis_index("mode"), lax.axis_index("node")
    _, _, pieces, piece, wide = gathered.shape
    rows, deep = pieces * piece, pieces // 2
    half = rows // 2
    last = deep - 1
    samples = coefs.shape[-1]
    across, sibling = (1 - g, me, c), (g, me, 1 - c)
    mine, theirs = [[side * deep + p for p in range(deep)] for side in (g, 1 - g)]

    def to(step):
        flipped, bit = 0, 1
        while bit < n:
            flipped = flipped + lax.rem(me // bit + step // bit, 2) * bit
            bit *= 2
        return flipped

    near, quarter, eighth = n // 2, n // 4, n // 8
    inner = lax.rem(me // near + me // quarter, 2)

    def far(q):
        return near + quarter - 1 - q // 2 + lax.rem(q, 2) * quarter

    def relay(j):
        base = n - 1 - j
        return base + inner * (quarter * (1 - 2 * ((base // quarter) % 2)))

    def each(low, high, body):
        if high - low == 1:
            body(low)
        else:
            pl.loop(low, high)(body)

    def group(index):
        return index * eighth, (index + 1) * eighth

    def outside(*actions):
        @pl.when(inner == 0)
        def _():
            for action in actions:
                action()

    def inside(*actions):
        @pl.when(inner == 1)
        def _():
            for action in actions:
                action()

    def settle(block, sem):
        pltpu.make_async_copy(block, block, sem).wait()

    barrier = pltpu.get_barrier_semaphore()

    @pl.loop(1, n)
    def _(step):
        pl.semaphore_signal(barrier, inc=1, device_id=(g, to(step), c), device_id_type=MESH)
        pl.semaphore_signal(barrier, inc=1, device_id=(g, to(step), 1 - c), device_id_type=MESH)

    pl.semaphore_signal(barrier, inc=1, device_id=across, device_id_type=MESH)
    pl.semaphore_signal(barrier, inc=1, device_id=sibling, device_id_type=MESH)

    small = [
        pltpu.make_async_copy(scales, scale_all.at[me], small_sems.at[0]),
        pltpu.make_async_copy(mean, mean_all.at[c], small_sems.at[1]),
        pltpu.make_async_copy(seeds.at[:, pl.ds(pl.multiple_of(c * samples, 128), samples)], seed_row, small_sems.at[2]),
    ]
    for copy in small:
        copy.start()
    own_columns = pl.ds(pl.multiple_of(me * wide, 128), wide)
    for k in range(pieces):
        pltpu.make_async_copy(
            basis.at[pl.ds(k * piece, piece), own_columns], gathered.at[c, me, k], own_sem.at[0]).start()
    for copy in small:
        copy.wait()
    pl.semaphore_wait(barrier, 2 * n)

    def net(step, owner, k, send_sem, recv_sem):
        peer = to(step)
        return pltpu.make_async_remote_copy(
            src_ref=basis.at[pl.ds(pl.multiple_of(k * piece, 8), piece), pl.ds(pl.multiple_of(peer * wide, 128), wide)],
            dst_ref=gathered.at[c, owner, k],
            send_sem=send_sem, recv_sem=recv_sem, device_id=(g, peer, c), device_id_type=MESH)

    def far_copy(step, owner, p):
        return net(step, owner, mine[p], net_send.at[0], far_recv.at[p, step - near])

    def near_copy(step, owner, k):
        return net(step, owner, k, net_send.at[1], near_recv.at[k // deep, step])

    def extra_copy(j, owner):
        return net(relay(j), owner, theirs[last], net_send.at[2], extra_recv.at[j - 3 * eighth])

    def scale_copy(step, owner):
        return pltpu.make_async_remote_copy(
            src_ref=scale_all.at[me], dst_ref=scale_all.at[owner],
            send_sem=scale_send.at[0], recv_sem=scale_recv.at[step], device_id=(g, to(step), c), device_id_type=MESH)

    def row_copy(j, owner, p):
        block = gathered.at[c, owner, mine[p]]
        sem = row_send.at[(j - 3 * eighth + near) // near]
        return pltpu.make_async_remote_copy(
            src_ref=block, dst_ref=block,
            send_sem=sem, recv_sem=row_recv.at[2 * p // deep, relay(j) - near], device_id=across, device_id_type=MESH)

    def core_copy(step, owner, k, h, side):
        block = gathered.at[side, owner, k]
        return pltpu.make_async_remote_copy(
            src_ref=block, dst_ref=block,
            send_sem=core_send.at[0], recv_sem=core_recv.at[h, step],
            device_id=sibling, device_id_type=MESH)

    def part_copy(step, owner, source, target):
        return pltpu.make_async_remote_copy(
            src_ref=parts.at[c, me], dst_ref=parts.at[source, owner],
            send_sem=part_send.at[lax.rem(target + c, 2)], recv_sem=part_recv.at[lax.rem(source + target, 2)],
            device_id=(g, to(step), target), device_id_type=MESH)

    mean_copy = lambda side: pltpu.make_async_remote_copy(
        src_ref=mean_all.at[c], dst_ref=mean_all.at[side], send_sem=mean_sems.at[0], recv_sem=mean_sems.at[1],
        device_id=sibling, device_id_type=MESH)

    @pl.loop(1, n)
    def _(step):
        scale_copy(step, me).start()

    mean_copy(c).start()

    @pl.loop(0, near)
    def _(q):
        for p in range(deep):
            far_copy(far(q), me, p).start()

    inside(lambda: each(*group(3), lambda j: extra_copy(j, me).start()))

    @pl.loop(quarter, near)
    def _(step):
        for k in range(pieces):
            near_copy(step, me, k).start()

    @pl.loop(1, quarter)
    def _(step):
        for k in range(pieces):
            near_copy(step, me, k).start()

    settle(gathered.at[c, me], own_sem.at[0])
    for k in range(pieces):
        core_copy(0, me, k, k // deep, c).start()

    seed_terms = seed_row[...] * jnp.int32(-1640531527)
    lanes = min(512, samples)
    tiles = half // 16

    def draw_half(owner, side):
        @pl.loop(0, tiles)
        def _(tile):
            first = owner * rows + side * half + tile * 16
            ids = lax.broadcasted_iota(jnp.int32, (16, lanes), 0) + first
            counters = ids * jnp.int32(2 * 668265261 - 2**32 if 2 * 668265261 >= 2**31 else 2 * 668265261)
            for start in range(0, samples, lanes):
                high, low = split(normals(seed_terms[:, start:start + lanes], counters))
                for part, values in enumerate((high, low, high)):
                    here = pl.ds(pl.multiple_of((3 * side + part) * half + tile * 16, 16), 16)
                    coefs[owner, here, start:start + lanes] = values

    def draw(owner):
        draw_half(owner, 0)
        draw_half(owner, 1)

    def accumulate(owner, first_row, depth, first):
        columns = min(1024, samples)

        @pl.loop(0, samples // columns)
        def _(tile):
            here = pl.ds(pl.multiple_of(tile * columns, 128), columns)
            product = jnp.dot(lhs[:, 0:depth], coefs[owner, pl.ds(first_row, depth), here], preferred_element_type=jnp.float32)
            if first:
                for spot, side in enumerate((1 - c, c)):
                    shift = jnp.broadcast_to(mean_all[side], (8, wide)).T[:, :1]
                    total[spot * wide:(spot + 1) * wide, here] = product[spot * wide:(spot + 1) * wide] + shift
            else:
                total[:, here] += product

    def conclude(owner, first_row, depth):
        columns = min(256, samples)
        for start in range(0, samples, columns):
            here = slice(start, start + columns)
            product = jnp.dot(lhs[:, 0:depth], coefs[owner, pl.ds(first_row, depth), here], preferred_element_type=jnp.float32)
            values = jnp.exp(total[:, here] + product)
            staged[:, here] = values[0:wide]
            modulus[c, :, here] = values[wide:2 * wide]
            parts[c, me, :, here] = jnp.sum(values, axis=0, keepdims=True)

    def scaled(step):
        scale_copy(step, to(step)).wait_recv()
        return step

    def arrived(step, owner, h):
        settle(gathered.at[1 - c, owner, pl.ds(h * deep, deep)], core_recv.at[h, step])

    def multiply(step, first):
        owner = to(step)
        for h in range(2):
            arrived(step, owner, h)
        for spot, side in enumerate((1 - c, c)):
            block = gathered[side, owner].reshape(rows, wide)
            high, low = split(block.T * scale_all[owner])
            for h in range(2):
                for part, values in enumerate((high, high, low)):
                    at = (3 * h + part) * half
                    lhs[spot * wide:(spot + 1) * wide, at:at + half] = values[:, h * half:(h + 1) * half]
        accumulate(owner, 0, 3 * rows, first)

    def multiply_half(step, h, final=False):
        owner = to(step)
        arrived(step, owner, h)
        scale_row = jnp.where(h == 0, scale_all[owner][:, 0:half], scale_all[owner][:, half:rows])
        for spot, side in enumerate((1 - c, c)):
            block = gathered[side, owner, pl.ds(h * deep, deep)].reshape(half, wide)
            high, low = split(block.T * scale_row)
            for part, values in enumerate((high, high, low)):
                lhs[spot * wide:(spot + 1) * wide, part * half:(part + 1) * half] = values
        first_row = pl.multiple_of(h * (3 * half), 16)
        if final:
            conclude(owner, first_row, 3 * half)
        else:
            accumulate(owner, first_row, 3 * half, False)

    def forward(j, p, relayed=True):
        step = relay(j)
        owner = to(step)
        far_copy(step, owner, p).wait_recv()
        if relayed:
            row_copy(j, owner, p).start()
        core_copy(step, owner, mine[p], g, c).start()

    def finish(j, ps, relayed):
        step = relay(j)
        owner = to(step)
        settle(gathered.at[c, owner, pl.ds(theirs[ps[0]], relayed)], row_recv.at[2 * ps[0] // deep, step - near])
        if relayed < len(ps):
            extra_copy(j, owner).wait_recv()
        for p in ps:
            core_copy(step, owner, theirs[p], 1 - g, c).start()

    def forwards(index, *ps):
        for p in ps:
            each(*group(index), lambda j: forward(j, p))

    def forward_last(index):
        each(*group(index), lambda j: forward(j, last, False))

    def finishes(index, *halves, relayed=deep // 2):
        for ps in halves:
            each(*group(index), lambda j: finish(j, ps, relayed))

    def share(step, h):
        owner = to(step)
        settle(gathered.at[c, owner, pl.ds(h * deep, deep)], near_recv.at[h, step])
        for k in range(h * deep, (h + 1) * deep):
            core_copy(step, owner, k, h, c).start()

    def share_near(index, *hs):
        for h in hs:
            each(*group(index), lambda step: share(step, h))

    def draw_far(index, side):
        each(*group(index), lambda j: draw_half(to(relay(j)), side))

    def draw_near(index, side):
        each(*group(index), lambda step: draw_half(to(step), side))

    def use_far(index):
        each(*group(index), lambda j: multiply(scaled(relay(j)), False))

    def use_near(index, h):
        each(*group(index), lambda step: multiply_half(step if h else scaled(step), h))

    def use_mine(index):
        each(*group(index), lambda j: multiply_half(scaled(relay(j)), g))

    def use_theirs(index):
        each(*group(index), lambda j: multiply_half(relay(j), 1 - g))

    early, late = tuple(range(deep // 2)), tuple(range(deep // 2, deep))
    draw(me)
    each(1, quarter, lambda step: draw(to(step)))
    mean_copy(1 - c).wait_recv()
    multiply(0, True)
    inside(lambda: forwards(0, *early, *late))
    draw_far(0, 0)
    outside(lambda: forwards(0, *early))
    draw_far(0, 1)
    draw_far(1, 0)
    outside(lambda: forwards(0, *late))
    inside(lambda: finishes(0, early))
    draw_far(1, 1)
    outside(lambda: finishes(0, early))
    inside(lambda: finishes(0, late), lambda: forwards(1, *early))
    draw_near(2, 0)
    inside(lambda: forwards(1, *late))
    for h in range(2):
        each(1, quarter, lambda step: share(step, h))
    draw_near(2, 1)
    outside(lambda: finishes(0, late), lambda: forwards(1, *early))
    each(1, quarter, lambda step: multiply(scaled(step), False))
    inside(lambda: finishes(1, early))
    use_far(0)
    outside(lambda: forwards(1, *late))
    inside(lambda: finishes(1, late))
    draw_far(2, 0)
    outside(lambda: forwards(2, 0))
    draw_far(2, 1)
    outside(lambda: forwards(2, 1, 2), lambda: finishes(1, early))
    draw_near(3, 0)
    outside(lambda: forwards(2, 3), lambda: finishes(1, late))
    draw_near(3, 1)
    inside(lambda: forwards(2, *early))
    use_far(1)
    inside(lambda: forwards(2, 2))
    draw_far(3, 0)
    inside(lambda: forwards(2, 3))
    share_near(2, 0, 1)
    draw_far(3, 1)
    outside(lambda: finishes(2, early, late), lambda: forwards(3, 0, 1, 2))
    use_near(2, 0)
    outside(lambda: forwards(3, 3))
    use_near(2, 1)
    use_mine(2)
    inside(lambda: forwards(3, 0), lambda: finishes(2, early, late))
    share_near(3, 0)
    inside(lambda: forwards(3, 1))
    use_near(3, 0)
    inside(lambda: forwards(3, 2))
    use_theirs(2)
    inside(lambda: forward_last(3))
    outside(lambda: finishes(3, early))
    inside(lambda: share_near(3, 1), lambda: finishes(3, early))
    use_mine(3)
    outside(lambda: finishes(3, late), lambda: share_near(3, 1))
    inside(lambda: finishes(3, late, relayed=deep // 2 - 1))

    def use_last(turn, low, high, final=False):
        def body(step):
            picked = lax.rem(inner + turn, 2)
            multiply_half(picked * step + (1 - picked) * relay(step), picked + (1 - picked) * (1 - g), final)

        if high > low:
            each(low, high, body)

    end = 4 * eighth
    use_last(0, 3 * eighth, end)
    use_last(1, 3 * eighth, end - 1)
    use_last(1, end - 1, end, True)

    send_out = lambda half_index: pltpu.make_async_remote_copy(
        src_ref=staged, dst_ref=modulus.at[half_index], send_sem=out_sems.at[0], recv_sem=out_sems.at[1],
        device_id=sibling, device_id_type=MESH)

    @pl.loop(1, n)
    def _(step):
        part_copy(step, me, c, c).start()
        part_copy(step, me, c, 1 - c).start()

    part_copy(0, me, c, 1 - c).start()
    send_out(c).start()

    mean_copy(c).wait_send()
    settle(scale_all.at[0:n - 1], scale_send.at[0])
    settle(gathered.at[0, 0:near, 0:deep], net_send.at[0])
    settle(gathered.at[0, 0:near - 1], net_send.at[1])
    settle(gathered.at[0], core_send.at[0])
    settle(gathered.at[0, 0:3 * eighth, 0:deep], row_send.at[0])
    outside(lambda: settle(gathered.at[0, 0:eighth, 0:deep], row_send.at[1]))
    inside(lambda: settle(gathered.at[0, 0:eighth, 0:last], row_send.at[1]),
           lambda: settle(gathered.at[0, 0:eighth, 0], net_send.at[2]))
    settle(parts.at[0, 0:n - 1], part_send.at[0])
    settle(parts.at[0], part_send.at[1])
    settle(parts.at[0, 0:n - 1], part_recv.at[0])
    settle(parts.at[0], part_recv.at[1])

    for side in range(2):
        summed = jnp.zeros((1, samples), jnp.float32)
        for m in range(n):
            summed = summed + parts[side, m]
        means[:, side * samples:(side + 1) * samples] = summed / (n * 2 * wide)
    send_out(1 - c).wait_recv()
    send_out(c).wait_send()


def write_out(values, sums, modulus, means, sems):
    rows, samples = values.shape[1:]
    part = rows // 2
    copies = [pltpu.make_async_copy(sums, means, sems.at[4])]
    for side in range(2):
        for block in range(2):
            here = pl.ds(block * part, part)
            copies.append(pltpu.make_async_copy(
                values.at[side, here], modulus.at[here, side * samples:(side + 1) * samples], sems.at[2 * side + block]))
    for copy in copies:
        copy.start()
    for copy in copies:
        copy.wait()


def on_device(mode_basis, mode_scales, mean_log, sample_seeds):
    n = lax.axis_size("mode")
    rows, wide, all_samples = mode_scales.shape[0], mean_log.shape[0], sample_seeds.shape[0]
    piece, samples, near = rows // PIECES, all_samples // 2, n // 2
    vmem = pl.BlockSpec(memory_space=pltpu.VMEM)
    anywhere = pl.BlockSpec(memory_space=pl.ANY)
    dma = pltpu.SemaphoreType.DMA
    modulus, means = pl.pallas_call(
        functools.partial(kernel, n),
        out_shape=(
            pltpu.VMEM((2, wide, samples), jnp.float32),
            pltpu.VMEM((1, all_samples), jnp.float32),
        ),
        in_specs=[anywhere] * 4,
        out_specs=(vmem, vmem),
        scratch_shapes=[
            pltpu.VMEM((2, n, PIECES, piece, wide), jnp.float32),
            pltpu.VMEM((n, 1, rows), jnp.float32),
            pltpu.VMEM((2, 1, wide), jnp.float32),
            pltpu.VMEM((1, samples), jnp.int32),
            pltpu.VMEM((n, 3 * rows, samples), jnp.bfloat16),
            pltpu.VMEM((2 * wide, 3 * rows), jnp.bfloat16),
            pltpu.VMEM((2 * wide, samples), jnp.float32),
            pltpu.VMEM((wide, samples), jnp.float32),
            pltpu.VMEM((2, n, 1, samples), jnp.float32),
            dma((2, near)), dma((PIECES // 2, near)), dma((n // 8,)), dma((3,)), dma((2, near)), dma((2,)), dma((2, n)), dma((1,)),
            dma((1,)), dma((n,)), dma((2,)), dma((1,)), dma((2,)), dma((2,)), dma((2,)), dma((3,)),
        ],
        compiler_params=pltpu.CompilerParams(
            collective_id=0, has_side_effects=True, vmem_limit_bytes=52 * 1024 * 1024
        ),
    )(mode_basis, mode_scales[None, :], mean_log[None, :], sample_seeds[None, :])
    return pl.pallas_call(
        write_out,
        out_shape=(
            jax.ShapeDtypeStruct((wide, all_samples), jnp.float32),
            jax.ShapeDtypeStruct((1, all_samples), jnp.float32),
        ),
        in_specs=[vmem, vmem],
        out_specs=(anywhere, anywhere),
        scratch_shapes=[dma((5,))],
        compiler_params=pltpu.CompilerParams(vmem_limit_bytes=1024 * 1024),
    )(*(pltpu.with_memory_space_constraint(array, pltpu.VMEM) for array in (modulus, means)))


def solution(mesh):
    def call(*arrays):
        modulus, means = on_device(*arrays)
        return modulus, means[0]

    return jax.shard_map(
        call,
        mesh=mesh,
        in_specs=(P("mode", "node"), P("mode"), P(("node", "mode")), P("grp")),
        out_specs=(P(("node", "mode"), "grp"), P("grp")),
        check_vma=False,
    )
```
